256 devices in a mesh: dp: 32 (over z, y_hi, core), tensor: 8 (over x, y_lo).
Axes of the slice: x: 4, y: 4 (y_hi: 2, y_lo: 2; y = y_hi * 2 + y_lo), z: 8, core: 2. Of those that a mesh axis runs over, the one named last changes fastest.
Arguments:
- tokens: bfloat16 [128, 576, 1024], P('dp', 'tensor'), may hold values from -150 to 150
- cotangent: bfloat16 [128, 576, 1024], P('dp', 'tensor'), may hold values from -6 to 6
- dispatch_weight: bfloat16 [1024, 64], replicated, may hold values from -3 to 3
- w_in: bfloat16 [64, 1024, 4096], P('dp', None, 'tensor'), may hold values from -0.1875 to 0.1875
- w_out: bfloat16 [64, 4096, 1024], P('dp', 'tensor'), may hold values from -0.09375 to 0.09375
Outputs:
- grad_tokens: bfloat16 [128, 576, 1024], P('dp', 'tensor')
- grad_router: float32 [1024, 64], replicated
- grad_w_in: bfloat16 [64, 1024, 4096], P('dp', None, 'tensor')
- grad_w_out: bfloat16 [64, 4096, 1024], P('dp', 'tensor')
The draws below stay inside these ranges and needn't reach their ends.
All inputs are finite; a program needn't handle non-finite values.
Results may differ from the reference program's by a relative error of at most 0.0079.
Values may be sent and summed in bfloat16 or wider, within the bound.
No kernel may reach another device: no remote copies, remote signals or barrier semaphores. Data moves between devices by JAX's collectives and lax.ppermute only.
A program may use at most 64 MiB of HBM per device.

```python
import math
import jax
import jax.numpy as jnp
from jax import lax

D = 1024
FF = 4096
EXPERTS = 64
IMAGES = 128
SEQ = 576


def drawn_pair(key):
    router_key = jax.random.fold_in(key, 101)
    token_key = jax.random.fold_in(key, 102)
    router = jnp.clip(jax.random.normal(router_key, (D, EXPERTS), jnp.float32), -6.0, 6.0) * (3.0 / math.sqrt(D))
    base = jnp.clip(jax.random.normal(token_key, (IMAGES, SEQ, D), jnp.float32), -6.0, 6.0)
    position = jnp.arange(SEQ, dtype=jnp.float32) / max(SEQ - 1, 1)
    base = base * (0.6 * 3.0 ** position)[None, :, None]
    return (base, router)


def draw_tokens(key, part):
    return drawn_pair(key)[0].astype(jnp.bfloat16)


def draw_dispatch_weight(key, part):
    return drawn_pair(key)[1].astype(jnp.bfloat16)


def block_levels(own_key, dims, cuts, smallest, largest):
    gain = 1.0
    for axis_at, shards_of in cuts:
        draws = jax.random.uniform(jax.random.fold_in(jax.random.fold_in(own_key, 6), axis_at), (shards_of,), jnp.float32, smallest / len(cuts), largest / len(cuts))
        gain = gain * jnp.repeat(jnp.exp(draws), dims[axis_at] // shards_of).reshape((-1,) + (1,) * (len(dims) - 1 - axis_at))
    return gain


def bell_draw(own_key, dims, width, reach, split=(), kind=jnp.bfloat16):
    entries = jax.random.normal(own_key, dims, jnp.float32) * width
    if len(split) > 0:
        entries = block_levels(own_key, dims, split, -0.22, 0.18) * entries
    return jnp.clip(entries, min=-reach, max=reach).astype(kind)


def setup_inputs(seed: int = 0) -> dict:
    seeds = jax.random.split(jax.random.key(seed), 6)
    tokens = draw_tokens(jax.random.fold_in(seeds[5], 71), 0)
    cotangent = bell_draw(seeds[1], (IMAGES, SEQ, D), 1.0, 6.0, ((0, 32), (1, 8)))
    dispatch_weight = draw_dispatch_weight(jax.random.fold_in(seeds[5], 71), 0)
    w_in = bell_draw(seeds[3], (EXPERTS, D, FF), D ** -0.5, 0.1875, ((0, 32), (2, 8)))
    w_out = bell_draw(seeds[4], (EXPERTS, FF, D), FF ** -0.5, 0.09375, ((0, 32), (1, 8)))
    return dict(tokens=tokens, cotangent=cotangent, dispatch_weight=dispatch_weight, w_in=w_in, w_out=w_out)


def rounded(values):
    return lax.optimization_barrier(values.astype(jnp.bfloat16)).astype(jnp.float32)

def expert_forward(operands):
    slot_rows, first_mat, second_mat = operands
    pre_act = jnp.einsum('id,df->if', slot_rows, first_mat.astype(jnp.float32))
    hidden_low = rounded(jax.nn.gelu(pre_act))
    return jnp.einsum('if,fd->id', hidden_low, second_mat.astype(jnp.float32)).astype(jnp.bfloat16)

def expert_backward(operands):
    slot_rows, grad_rows, first_mat, second_mat = operands
    first_wide = first_mat.astype(jnp.float32)
    second_wide = second_mat.astype(jnp.float32)
    pre_act = jnp.einsum('id,df->if', slot_rows, first_wide)
    hidden_act, gelu_back = jax.vjp(jax.nn.gelu, pre_act)
    hidden_low = rounded(hidden_act)
    grad_hidden = jnp.einsum('id,fd->if', grad_rows, second_wide)
    grad_pre = rounded(gelu_back(grad_hidden)[0])
    grad_second = jnp.einsum('if,id->fd', hidden_low, grad_rows).astype(jnp.bfloat16)
    grad_first = jnp.einsum('id,if->df', slot_rows, grad_pre).astype(jnp.bfloat16)
    grad_slot = jnp.einsum('if,df->id', grad_pre, first_wide).astype(jnp.bfloat16)
    return (grad_first, grad_second, grad_slot)

def reference(tokens, cotangent, dispatch_weight, w_in, w_out):
    token_vals = tokens.astype(jnp.float32)
    grad_vals = cotangent.astype(jnp.float32)
    router = dispatch_weight.astype(jnp.float32)
    logits = jnp.einsum('isd,de->ise', token_vals, router)
    dispatch = jax.nn.softmax(logits, axis=1)
    combine = jax.nn.softmax(logits, axis=2)
    dispatch_low = rounded(dispatch)
    combine_low = rounded(combine)
    slot_inputs = rounded(jnp.einsum('ise,isd->ied', dispatch_low, token_vals))
    slot_major = jnp.transpose(slot_inputs, (1, 0, 2))
    slot_outputs = lax.map(expert_forward, (slot_major, w_in, w_out))
    slot_outputs = jnp.transpose(slot_outputs, (1, 0, 2)).astype(jnp.float32)
    grad_combine = jnp.einsum('isd,ied->ise', grad_vals, slot_outputs)
    grad_slots_out = rounded(jnp.einsum('ise,isd->ied', combine_low, grad_vals))
    grad_major = jnp.transpose(grad_slots_out, (1, 0, 2))
    grad_w_in, grad_w_out, grad_slots_in = lax.map(expert_backward, (slot_major, grad_major, w_in, w_out))
    grad_slots_in = jnp.transpose(grad_slots_in, (1, 0, 2)).astype(jnp.float32)
    grad_dispatch = jnp.einsum('isd,ied->ise', token_vals, grad_slots_in)
    row_dot = lax.optimization_barrier(jnp.sum(grad_combine * combine, axis=2, keepdims=True))
    column_dot = lax.optimization_barrier(jnp.sum(grad_dispatch * dispatch, axis=1, keepdims=True))
    grad_logits = rounded(combine * (grad_combine - row_dot) + dispatch * (grad_dispatch - column_dot))
    grad_tokens = (jnp.einsum('ise,ied->isd', dispatch_low, grad_slots_in) + jnp.einsum('ise,de->isd', grad_logits, router)).astype(jnp.bfloat16)
    grad_router = jnp.einsum('isd,ise->de', token_vals, grad_logits)
    return (grad_tokens, grad_router, grad_w_in, grad_w_out)
```

```python
import jax
import jax.numpy as jnp
from jax import lax
from jax.sharding import PartitionSpec as P

NARROW = jnp.bfloat16
WIDE = jnp.float32


def exchanged(blocks, axis):
    return lax.all_to_all(blocks, axis, split_axis=0, concat_axis=0, tiled=True)


def pieces(x, count):
    found = []
    for _ in range(count):
        piece = lax.reduce_precision(x, exponent_bits=8, mantissa_bits=7)
        found.append(piece.astype(NARROW))
        x = x - piece
    return found


def with_extra_rows(blocks, rows):
    extra = jnp.stack(rows + [jnp.zeros_like(rows[0])] * (8 - len(rows)))
    extra = jnp.broadcast_to(extra[None], (blocks.shape[0], *extra.shape))
    return jnp.concatenate([blocks, extra], axis=1)


def feature_blocks(x, count):
    rows, width = x.shape
    return jnp.moveaxis(x.reshape(rows, count, width // count), 1, 0)


def joined_features(blocks):
    count, rows, width = blocks.shape
    return jnp.moveaxis(blocks, 0, 1).reshape(rows, count * width)


def on_device(tokens, cotangent, dispatch_weight, w_in, w_out):
    images, seq, width = tokens.shape
    slots = dispatch_weight.shape[1]
    parts = lax.axis_size("tensor")
    groups = lax.axis_size("dp")
    own = slots // groups
    rows = slots * images
    block = width // parts

    logits = jnp.einsum("isd,de->eis", tokens, dispatch_weight, preferred_element_type=WIDE)
    high, low = pieces(jnp.max(logits, axis=2), 2)
    local_top = high.astype(WIDE) + low.astype(WIDE)
    weight = jnp.exp(logits - local_top[:, :, None])
    local_total = jnp.sum(weight, axis=2)
    combine = jax.nn.softmax(logits, axis=0)
    partial_in = jnp.einsum("eis,isd->eid", weight.astype(NARROW), tokens, preferred_element_type=WIDE)
    partial_back = jnp.einsum(
        "eis,isd->eid", combine.astype(NARROW), cotangent, preferred_element_type=WIDE
    )
    sent = jnp.concatenate(
        [
            feature_blocks(partial_in.reshape(rows, width), parts),
            feature_blocks(partial_back.reshape(rows, width), parts),
        ],
        axis=2,
    ).astype(NARROW)
    stats = [high.reshape(rows), low.reshape(rows), *pieces(local_total.reshape(rows), 2)]
    arrived = exchanged(with_extra_rows(sent, stats), "tensor")

    seen = arrived[:, rows : rows + 4, :].astype(WIDE)
    tops = seen[:, 0] + seen[:, 1]
    top = jnp.max(tops, axis=0)
    factor = jnp.exp(tops - top)
    total = jnp.sum(factor * (seen[:, 2] + seen[:, 3]), axis=0)
    factor = factor / total
    body = arrived[:, :rows].astype(WIDE)
    slot_part = jnp.sum(body[:, :, :block] * factor[:, :, None], axis=0)
    back_part = jnp.sum(body[:, :, block:], axis=0)
    both = jnp.concatenate([slot_part, back_part], axis=1).astype(NARROW)
    arrived = exchanged(both.reshape(groups, own * images, 2 * block), "dp")
    ordered = jnp.moveaxis(arrived.reshape(groups, own, images, 2 * block), 1, 0).reshape(
        rows, 2 * block
    )
    arrived = exchanged(jnp.broadcast_to(ordered[None], (parts, *ordered.shape)), "tensor")
    total_images = groups * images
    slot_inputs = joined_features(arrived[:, :, :block]).reshape(own, total_images, width)
    grad_slots_out = joined_features(arrived[:, :, block:]).reshape(own, total_images, width)

    pre_act = jnp.einsum("eid,edf->eif", slot_inputs, w_in, preferred_element_type=WIDE)
    hidden_act, gelu_back = jax.vjp(jax.nn.gelu, pre_act)
    hidden_low = hidden_act.astype(NARROW)
    slot_outputs = jnp.einsum("eif,efd->eid", hidden_low, w_out, preferred_element_type=WIDE)
    grad_hidden = jnp.einsum("eid,efd->eif", grad_slots_out, w_out, preferred_element_type=WIDE)
    grad_pre = gelu_back(grad_hidden)[0].astype(NARROW)
    grad_slots_in = jnp.einsum("eif,edf->eid", grad_pre, w_in, preferred_element_type=WIDE)
    sent = jnp.concatenate(
        [
            feature_blocks(slot_outputs.reshape(rows, width), parts),
            feature_blocks(grad_slots_in.reshape(rows, width), parts),
        ],
        axis=2,
    ).astype(NARROW)
    arrived = exchanged(sent, "tensor")
    both = jnp.sum(arrived.astype(WIDE), axis=0).astype(NARROW)
    both = jnp.moveaxis(both.reshape(own, groups, images, 2 * block), 0, 1)
    grad_w_out = jnp.einsum(
        "eif,eid->efd", hidden_low, grad_slots_out, preferred_element_type=WIDE
    ).astype(NARROW)
    grad_w_in = jnp.einsum(
        "eid,eif->edf", slot_inputs, grad_pre, preferred_element_type=WIDE
    ).astype(NARROW)
    arrived = exchanged(both.reshape(groups, own * images, 2 * block), "dp").reshape(rows, 2 * block)
    dot_part = jnp.sum(slot_part * arrived[:, block:].astype(WIDE), axis=1)
    sent = jnp.broadcast_to(arrived[None], (parts, *arrived.shape))
    arrived = exchanged(with_extra_rows(sent, pieces(dot_part, 3)), "tensor")
    column_dot = jnp.sum(arrived[:, rows : rows + 3].astype(WIDE), axis=(0, 1))
    slot_outputs = joined_features(arrived[:, :rows, :block]).reshape(slots, images, width)
    grad_slots_in = joined_features(arrived[:, :rows, block:]).reshape(slots, images, width)

    dispatch = jnp.exp(logits - top.reshape(slots, images, 1)) / total.reshape(slots, images, 1)
    grad_combine = jnp.einsum("isd,eid->eis", cotangent, slot_outputs, preferred_element_type=WIDE)
    grad_dispatch = jnp.einsum("isd,eid->eis", tokens, grad_slots_in, preferred_element_type=WIDE)
    row_dot = jnp.sum(grad_combine * combine, axis=0, keepdims=True)
    grad_logits = (
        combine * (grad_combine - row_dot)
        + dispatch * (grad_dispatch - column_dot.reshape(slots, images, 1))
    ).astype(NARROW)
    local_router = jnp.einsum("eis,isd->ed", grad_logits, tokens, preferred_element_type=WIDE)
    ranks = groups * parts
    piece = slots * width // ranks
    arrived = exchanged(local_router.reshape(ranks, piece // 128, 128), ("dp", "tensor"))
    owned = jnp.sum(arrived, axis=0)
    arrived = exchanged(jnp.broadcast_to(owned[None], (ranks, *owned.shape)), ("dp", "tensor"))
    grad_router = arrived.reshape(slots, width).T
    token_part = jnp.einsum(
        "eis,eid->isd", dispatch.astype(NARROW), grad_slots_in, preferred_element_type=WIDE
    )
    router_part = jnp.einsum(
        "eis,de->isd", grad_logits, dispatch_weight, preferred_element_type=WIDE
    )
    grad_tokens = (token_part + router_part).astype(NARROW)
    return (grad_tokens, grad_router, grad_w_in, grad_w_out)


def solution(mesh):
    return jax.shard_map(
        on_device,
        mesh=mesh,
        in_specs=(
            P("dp", "tensor", None),
            P("dp", "tensor", None),
            P(),
            P("dp", None, "tensor"),
            P("dp", "tensor", None),
        ),
        out_specs=(P("dp", "tensor", None), P(), P("dp", None, "tensor"), P("dp", "tensor", None)),
        check_vma=False,
    )
```

```python
import functools

import jax
import jax.numpy as jnp
from jax import lax
from jax.experimental import pallas as pl
from jax.experimental.pallas import tpu as pltpu
from jax.sharding import Mesh
from jax.sharding import PartitionSpec as P

NARROW = jnp.bfloat16
WIDE = jnp.float32
LANES = 128
EXTRA = 8
FAR = -1e30
MIDDLE = NARROW
DP = ("z", "y_hi", "core")
PLANE = ("y_hi", "tensor")
COLUMN = ("z", "core")


def dot(a, b, over_a=1, over_b=0):
    return lax.dot_general(a, b, (((over_a,), (over_b,)), ((), ())), preferred_element_type=WIDE)


def iota(shape, dim):
    return lax.broadcasted_iota(jnp.int32, shape, dim)


def pieces(x, count):
    found = []
    for _ in range(count):
        piece = x.astype(NARROW).astype(WIDE)
        found.append(piece)
        x = x - piece
    return found


def as_lanes(columns, rows):
    lane = iota((rows, LANES), 1)
    found = jnp.zeros((rows, LANES), WIDE)
    for k, column in enumerate(columns):
        found = jnp.where(lane == k, column, found)
    return found


def as_columns(lines):
    return jnp.concatenate([lines, jnp.zeros((LANES - lines.shape[0], lines.shape[1]), WIDE)]).T


def combine_of(masked):
    weight = jnp.exp(masked - jnp.max(masked, axis=0, keepdims=True))
    return weight / jnp.sum(weight, axis=0, keepdims=True)


def slot_rows(
    images, seq, parts, token_src, back_src, router_src, sent, scores, spread, tokens, cotangent, router, arrivals
):
    copies_in = [
        pltpu.make_async_copy(source, target, arrivals.at[k])
        for k, (source, target) in enumerate(
            ((router_src, router), (token_src, tokens), (back_src, cotangent))
        )
    ]
    for copy in copies_in:
        copy.start()
    copies_in[0].wait()
    slots, width = router.shape
    rows, count, block = slots * images, images * seq, width // parts
    copies = (iota((rows, slots), 0) // images == iota((rows, slots), 1)).astype(NARROW)
    spread[...] = dot(copies, router[...]).astype(NARROW)
    own = iota((rows, count), 0) % images == iota((rows, count), 1) // seq
    copies_in[1].wait()
    masked = jnp.where(own, dot(spread[...], tokens[...], 1, 1), FAR)
    scores[...] = masked
    high, low = pieces(jnp.max(masked, axis=1, keepdims=True), 2)
    weight = jnp.exp(masked - (high + low))
    total = jnp.sum(weight, axis=1, keepdims=True)
    stats = as_lanes([high, low, *pieces(total, 2)], rows)
    lines = stats.T[:EXTRA].astype(NARROW)
    first, second = (piece.astype(NARROW) for piece in pieces(weight, 2))
    part_in = dot(first, tokens[...]) + dot(second, tokens[...])
    copies_in[2].wait()
    part_back = dot(combine_of(masked).astype(NARROW), cotangent[...])
    for t in range(parts):
        sent[t, :rows, :block] = part_in[:, t * block : (t + 1) * block].astype(NARROW)
        sent[t, :rows, block:] = part_back[:, t * block : (t + 1) * block].astype(NARROW)
        sent[t, rows:, :] = lines


def joined_rows(arrived, both, exact, stats):
    parts, rows, block = arrived.shape[0], both.shape[0], exact.shape[1]
    seen = [arrived[t, rows:, :].astype(WIDE) for t in range(parts)]
    tops = [line[0:1] + line[1:2] for line in seen]
    top = functools.reduce(jnp.maximum, tops)
    factors = [jnp.exp(own - top) for own in tops]
    total = sum(f * (line[2:3] + line[3:4]) for f, line in zip(factors, seen))
    scale = as_columns(jnp.concatenate([f / total for f in factors]))
    zeros = [jnp.zeros_like(top)] * (EXTRA - 2)
    stats[...] = as_columns(jnp.concatenate([top, total, *zeros]))
    slot_part = jnp.zeros((rows, block), WIDE)
    back_part = jnp.zeros((rows, block), WIDE)
    for t in range(parts):
        slot_part += arrived[t, :rows, :block].astype(WIDE) * scale[:, t : t + 1]
        back_part += arrived[t, :rows, block:].astype(WIDE)
    exact[...] = slot_part
    both[:, :block] = slot_part.astype(NARROW)
    both[:, block:] = back_part.astype(NARROW)


def by_expert(own, images, rows):
    row, column = iota((rows, rows), 0), iota((rows, rows), 1)
    each = rows // own
    source = (row % each) // images * (own * images) + row // each * images + row % images
    return (column == source).astype(NARROW)


def by_group(own, images, rows):
    row, column = iota((rows, rows), 0), iota((rows, rows), 1)
    each = rows // own
    target = (column % each) // images * (own * images) + column // each * images + column % images
    return (row == target).astype(NARROW)


def sorted_copies(own, images, arrived, sent):
    rows = arrived.shape[0]
    ordered = dot(by_expert(own, images, rows), arrived[...]).astype(NARROW)
    for t in range(sent.shape[0]):
        sent[t] = ordered


def halves(arrived, first, last):
    parts, block = arrived.shape[0], arrived.shape[2] // 2
    return tuple(
        jnp.concatenate([arrived[t, first:last, k * block : (k + 1) * block] for t in range(parts)], axis=1)
        for k in range(2)
    )


def experts(arrived, w_in, w_out, sent, acts):
    parts, rows, block = arrived.shape[0], arrived.shape[1], arrived.shape[2] // 2
    own, hidden_width = w_in.shape[0], w_in.shape[2]
    each = rows // own
    root = (2.0 / jnp.pi) ** 0.5
    for e in range(own):
        mine = slice(e * each, (e + 1) * each)
        slot_in, back = halves(arrived, e * each, (e + 1) * each)
        v = dot(slot_in, w_in[e])
        grad_hidden = dot(back, w_out[e], 1, 1)
        t = jnp.tanh(root * (v + 0.044715 * (v * v * v)))
        half = 0.5 * (1.0 + t)
        low = (v * half).astype(NARROW)
        slope = half + 0.5 * v * (1.0 - t * t) * (root * (1.0 + 3 * 0.044715 * (v * v)))
        grad_low = (slope * grad_hidden).astype(NARROW)
        acts[mine, :hidden_width] = low
        acts[mine, hidden_width:] = grad_low
        slot_out = dot(low, w_out[e])
        grad_in = dot(grad_low, w_in[e], 1, 1)
        for p in range(parts):
            sent[p, mine, :block] = slot_out[:, p * block : (p + 1) * block].astype(NARROW)
            sent[p, mine, block:] = grad_in[:, p * block : (p + 1) * block].astype(NARROW)


def weight_grads(arrived, acts, grad_in, grad_out):
    own, hidden_width = grad_in.shape[0], grad_in.shape[2]
    each = arrived.shape[1] // own
    for e in range(own):
        mine = slice(e * each, (e + 1) * each)
        slot_in, back = halves(arrived, e * each, (e + 1) * each)
        grad_in[e] = dot(slot_in, acts[mine, hidden_width:], 0, 0).astype(NARROW)
        grad_out[e] = dot(acts[mine, :hidden_width], back, 0, 0).astype(NARROW)


def joined_results(own, images, arrived, both):
    rows = both.shape[0]
    total = arrived[0].astype(WIDE)
    for t in range(1, arrived.shape[0]):
        total += arrived[t].astype(WIDE)
    both[...] = dot(by_group(own, images, rows), total.astype(NARROW)).astype(NARROW)


def dotted_copies(arrived, exact, sent):
    rows, block = exact.shape
    column = jnp.sum(exact[...] * arrived[:, block:].astype(WIDE), axis=1, keepdims=True)
    lines = as_lanes(pieces(column, 3), rows).T[:EXTRA].astype(NARROW)
    for t in range(sent.shape[0]):
        sent[t, :rows, :] = arrived[...]
        sent[t, rows:, :] = lines


def softmax_grads(
    images, arrived, tokens, cotangent, scores, stats, left, router
):
    parts, rows = arrived.shape[0], scores.shape[0]
    slots = rows // images
    slot_out, grad_in = halves(arrived, 0, rows)
    lines = arrived[0, rows:, :].astype(WIDE)
    for t in range(1, parts):
        lines += arrived[t, rows:, :].astype(WIDE)
    column_dot = jnp.sum(as_columns(lines)[:, :EXTRA], axis=1, keepdims=True)
    masked = scores[...]
    dispatch = jnp.exp(masked - stats[:, 0:1]) / stats[:, 1:2]
    combine = combine_of(masked)
    grad_combine = dot(slot_out, cotangent[...], 1, 1)
    grad_dispatch = dot(grad_in, tokens[...], 1, 1)
    row_dot = jnp.sum(grad_combine * combine, axis=0, keepdims=True)
    grad_logits = (
        combine * (grad_combine - row_dot) + dispatch * (grad_dispatch - column_dot)
    ).astype(NARROW)
    merge = (iota((slots, rows), 1) // images == iota((slots, rows), 0)).astype(NARROW)
    by_slot = dot(dot(merge, grad_logits).astype(NARROW), tokens[...])
    count, high, wide = router.shape
    across = by_slot.shape[1] // wide
    for k in range(count):
        down, right = k // across * high, k % across * wide
        router[k] = by_slot[down : down + high, right : right + wide].astype(router.dtype)
    left[:rows, :] = dispatch.astype(NARROW)
    left[rows:, :] = grad_logits


def token_grads(arrived, left, spread, grad_tokens):
    _, grad_in = halves(arrived, 0, spread.shape[0])
    right = jnp.concatenate([grad_in, spread[...]])
    grad_tokens[...] = dot(left[...], right, 0, 0).astype(NARROW)


def summed_copies(arrived, sent):
    total = arrived[0].astype(WIDE)
    for t in range(1, arrived.shape[0]):
        total += arrived[t].astype(WIDE)
    for t in range(sent.shape[0]):
        sent[t] = total.astype(sent.dtype)


def placed(arrived, router):
    count, high, wide = arrived.shape
    across = router.shape[1] // wide
    for k in range(count):
        down, right = k // across * high, k % across * wide
        router[down : down + high, right : right + wide] = arrived[k].astype(router.dtype)


def local(body, outs, flops, *args, limit=12, space=pltpu.VMEM, scratch=()):
    held = pl.BlockSpec(memory_space=pltpu.VMEM)
    moved = sum(a.size * a.dtype.itemsize for a in (*args, *outs))
    return pl.pallas_call(
        body,
        out_shape=outs,
        in_specs=[pl.BlockSpec(memory_space=space)] * len(args),
        scratch_shapes=scratch,
        out_specs=tuple([held] * len(outs)),
        cost_estimate=pl.CostEstimate(flops=flops, bytes_accessed=moved, transcendentals=0),
        compiler_params=pltpu.CompilerParams(vmem_limit_bytes=limit << 20),
    )(*args)


def shaped(shape, dtype=NARROW):
    return jax.ShapeDtypeStruct(shape, dtype)


def exchanged(blocks, axis):
    return lax.all_to_all(blocks, axis, split_axis=0, concat_axis=0, tiled=True)


def on_device(tokens, cotangent, dispatch_weight, w_in, w_out):
    images, seq, width = tokens.shape
    slots = dispatch_weight.shape[1]
    parts, groups = lax.axis_size("tensor"), lax.axis_size(DP)
    own, hidden_width = slots // groups, w_in.shape[2]
    rows, block, count = slots * images, width // parts, images * seq
    tokens, cotangent = tokens.reshape(count, width), cotangent.reshape(count, width)
    pair = 2 * block

    sent, scores, spread = local(
        functools.partial(slot_rows, images, seq, parts),
        (
            shaped((parts, rows + EXTRA, pair)),
            shaped((rows, count), WIDE),
            shaped((rows, width)),
        ),
        6 * rows * count * width,
        tokens,
        cotangent,
        dispatch_weight.T,
        limit=56,
        space=pltpu.HBM,
        scratch=(
            pltpu.VMEM(tokens.shape, NARROW),
            pltpu.VMEM(tokens.shape, NARROW),
            pltpu.VMEM((slots, width), NARROW),
            pltpu.SemaphoreType.DMA((3,)),
        ),
    )
    arrived = exchanged(sent, "tensor")
    both, exact, stats = local(
        joined_rows,
        (shaped((rows, pair)), shaped((rows, block), WIDE), shaped((rows, LANES), WIDE)),
        4 * rows * width,
        arrived,
    )
    arrived = exchanged(both.reshape(groups, own * images, pair), DP).reshape(rows, pair)
    (sent,) = local(
        functools.partial(sorted_copies, own, images),
        (shaped((parts, rows, pair)),),
        2 * rows * rows * pair,
        arrived,
    )
    arrived = exchanged(sent, "tensor")
    sent, acts = local(
        experts,
        (
            shaped((parts, rows, pair)),
            shaped((rows, 2 * hidden_width)),
        ),
        8 * rows * width * hidden_width,
        arrived,
        w_in,
        w_out,
    )
    back = exchanged(sent, "tensor")
    grad_w_in, grad_w_out = local(
        weight_grads,
        (shaped(w_in.shape), shaped(w_out.shape)),
        4 * rows * width * hidden_width,
        arrived,
        acts,
    )
    back, grad_w_in, grad_w_out = lax.optimization_barrier((back, grad_w_in, grad_w_out))
    (both,) = local(
        functools.partial(joined_results, own, images),
        (shaped((rows, pair)),),
        2 * rows * rows * pair,
        back,
    )
    arrived = exchanged(both.reshape(groups, own * images, pair), DP).reshape(rows, pair)
    (sent,) = local(
        dotted_copies, (shaped((parts, rows + EXTRA, pair)),), 4 * rows * width, arrived, exact
    )
    arrived = exchanged(sent, "tensor")
    plane = lax.axis_size(PLANE)
    across = width // LANES
    high = slots * across // plane
    left, router = local(
        functools.partial(softmax_grads, images),
        (shaped((2 * rows, count)), shaped((plane, high, LANES), MIDDLE)),
        4 * rows * count * width,
        arrived,
        tokens,
        cotangent,
        scores,
        stats,
    )
    (grad_tokens,) = local(
        token_grads,
        (shaped((count, width)),),
        4 * rows * count * width,
        arrived,
        left,
        spread,
    )
    column = lax.axis_size(COLUMN)
    (router,) = local(
        summed_copies,
        (shaped((column, high, LANES), MIDDLE),),
        slots * width,
        exchanged(router, PLANE),
    )
    (router,) = local(
        summed_copies,
        (shaped((plane, high, LANES), WIDE),),
        slots * width,
        exchanged(router, COLUMN),
    )
    (router,) = local(
        placed, (shaped((slots, width), WIDE),), slots * width, exchanged(router, PLANE)
    )
    grad_router = router.T
    return (grad_tokens.reshape(images, seq, width), grad_router, grad_w_in, grad_w_out)


def solution(mesh):
    depth = mesh.devices.shape[0] // 4
    fine = Mesh(
        mesh.devices.reshape(depth, 2, 2, mesh.devices.shape[1]), ("z", "y_hi", "core", "tensor")
    )
    return jax.shard_map(
        on_device,
        mesh=fine,
        in_specs=(
            P(DP, "tensor", None),
            P(DP, "tensor", None),
            P(),
            P(DP, None, "tensor"),
            P(DP, "tensor", None),
        ),
        out_specs=(P(DP, "tensor", None), P(), P(DP, None, "tensor"), P(DP, "tensor", None)),
        check_vma=False,
    )
```

```python
import functools

import jax
import jax.numpy as jnp
from jax import lax
from jax.experimental import pallas as pl
from jax.experimental.pallas import tpu as pltpu
from jax.sharding import Mesh
from jax.sharding import PartitionSpec as P

NARROW = jnp.bfloat16
WIDE = jnp.float32
LANES = 128
EXTRA = 8
DP = ("z", "y_hi", "core")
TENSOR = ("x", "y_lo")
PLANE = ("y_hi", "x", "y_lo")
COLUMN = ("z", "core")


def dot(a, b, over_a=1, over_b=0):
    return lax.dot_general(a, b, (((over_a,), (over_b,)), ((), ())), preferred_element_type=WIDE)


def iota(shape, dim):
    return lax.broadcasted_iota(jnp.int32, shape, dim)


def pieces(x, count):
    found = []
    for _ in range(count):
        piece = x.astype(NARROW).astype(WIDE)
        found.append(piece)
        x = x - piece
    return found


def as_lanes(columns):
    rows = columns[0].shape[0]
    lane = iota((rows, LANES), 1)
    found = jnp.zeros((rows, LANES), WIDE)
    for k, column in enumerate(columns):
        found = jnp.where(lane == k, column, found)
    return found


def as_lines(columns, width):
    square = as_lanes(columns)
    square = jnp.concatenate([square, jnp.zeros((LANES - square.shape[0], LANES), WIDE)])
    lines = square.T[:EXTRA]
    return jnp.concatenate([lines, jnp.zeros((EXTRA, width - LANES), WIDE)], axis=1)


def as_columns(lines, rows):
    lines = lines[:, :LANES]
    return jnp.concatenate([lines, jnp.zeros((LANES - EXTRA, LANES), WIDE)]).T[:rows]


def selection(size, source):
    return (iota((size, size), 1) == source(iota((size, size), 0))).astype(NARROW)


def turned(size, outer, inner, unit):
    def source(row):
        a = row // unit % outer
        b = row // (unit * outer) % inner
        rest = row // (unit * outer * inner)
        return ((rest * outer + a) * inner + b) * unit + row % unit

    return selection(size, source)


def combine_of(scores):
    weight = jnp.exp(scores - jnp.max(scores, axis=0, keepdims=True))
    return weight / jnp.sum(weight, axis=0, keepdims=True)


def image_tokens(gathered):
    seq = gathered.shape[1] // 2
    return tuple(
        jnp.concatenate([gathered[k, f * seq : (f + 1) * seq, :] for k in range(gathered.shape[0])])
        for f in range(2)
    )


def slot_rows(planes, cores, own, gathered, router, sent, kept, scores, stats, ordered):
    slots, width = router.shape
    half = width // 2
    tokens, cotangent = image_tokens(gathered)
    ordered[...] = dot(turned(slots, planes, cores, own), router[...]).astype(NARROW)
    logits = dot(ordered[...], tokens, 1, 1)
    scores[...] = logits
    high, low = pieces(jnp.max(logits, axis=1, keepdims=True), 2)
    weight = jnp.exp(logits - (high + low))
    total = jnp.sum(weight, axis=1, keepdims=True)
    stats[...] = as_lanes([high + low, total])
    first, second = (piece.astype(NARROW) for piece in pieces(weight, 2))
    part_in = dot(first, tokens) + dot(second, tokens)
    part_back = dot(combine_of(logits).astype(NARROW), cotangent)
    lower = lax.axis_index("y_lo") == 0
    for k, part in enumerate((part_in, part_back)):
        mine = slice(k * slots, (k + 1) * slots)
        kept[mine, :] = jnp.where(lower, part[:, :half], part[:, half:])
        sent[mine, :] = jnp.where(lower, part[:, half:], part[:, :half]).astype(NARROW)
    sent[2 * slots :, :] = as_lines([high, low, *pieces(total, 2)], half).astype(NARROW)


def joined_rows(planes, own, arrived, kept, local_stats, both, exact, stats):
    slots = exact.shape[0]
    there = as_columns(arrived[2 * slots :, :].astype(WIDE), slots)
    top_here, total_here = local_stats[:, 0:1], local_stats[:, 1:2]
    top_there, total_there = there[:, 0:1] + there[:, 1:2], there[:, 2:3] + there[:, 3:4]
    top = jnp.maximum(top_here, top_there)
    here, there = jnp.exp(top_here - top), jnp.exp(top_there - top)
    total = here * total_here + there * total_there
    stats[...] = as_lanes([top, total])
    slot_part = kept[:slots, :] * (here / total) + arrived[:slots, :].astype(WIDE) * (there / total)
    back_part = kept[slots:, :] + arrived[slots : 2 * slots, :].astype(WIDE)
    exact[...] = slot_part
    narrow = jnp.concatenate([slot_part, back_part]).astype(NARROW)
    unit = planes * own
    both[...] = dot(turned(2 * slots, 2, slots // unit, unit), narrow).astype(NARROW)


def sorted_copies(planes, own, arrived, sent):
    rows = arrived.shape[0]
    unit = 2 * planes * own
    ordered = dot(turned(rows, rows // unit, unit, 1), arrived[...]).astype(NARROW)
    ordered = jnp.concatenate([ordered[: rows // 2], ordered[rows // 2 :]], axis=1)
    high = sent.shape[1]
    for k in range(sent.shape[0]):
        first = k // (sent.shape[0] // planes) * high
        sent[k] = ordered[first : first + high]


def expert_rows(arrived, own, e):
    each = arrived.shape[1] // own
    half = arrived.shape[2] // 2
    return tuple(
        jnp.concatenate(
            [
                jnp.concatenate(
                    [
                        arrived[j + h, e * each : (e + 1) * each, k * half : (k + 1) * half]
                        for h in range(2)
                    ],
                    axis=1,
                )
                for j in range(0, arrived.shape[0], 2)
            ]
        )
        for k in range(2)
    )


def experts(arrived, w_in, w_out, sent, acts):
    own, hidden_width = w_in.shape[0], w_in.shape[2]
    each, high, half = acts.shape[0] // own, arrived.shape[1] // own, arrived.shape[2] // 2
    root = (2.0 / jnp.pi) ** 0.5
    for e in range(own):
        mine = slice(e * each, (e + 1) * each)
        there = slice(e * high, (e + 1) * high)
        slot_in, back = expert_rows(arrived, own, e)
        v = dot(slot_in, w_in[e])
        grad_hidden = dot(back, w_out[e], 1, 1)
        t = jnp.tanh(root * (v + 0.044715 * (v * v * v)))
        upper = 0.5 * (1.0 + t)
        low = (v * upper).astype(NARROW)
        slope = upper + 0.5 * v * (1.0 - t * t) * (root * (1.0 + 3 * 0.044715 * (v * v)))
        grad_low = (slope * grad_hidden).astype(NARROW)
        acts[mine, :hidden_width] = low
        acts[mine, hidden_width:] = grad_low
        slot_out = dot(low, w_out[e]).astype(NARROW)
        grad_in = dot(grad_low, w_in[e], 1, 1).astype(NARROW)
        for k in range(sent.shape[0]):
            y, p = k // 2 * high, k % 2 * half
            sent[k, there, :half] = slot_out[y : y + high, p : p + half]
            sent[k, there, half:] = grad_in[y : y + high, p : p + half]


def weight_grads(arrived, acts, grad_in, grad_out):
    own, hidden_width = grad_in.shape[0], grad_in.shape[2]
    each = acts.shape[0] // own
    for e in range(own):
        mine = slice(e * each, (e + 1) * each)
        slot_in, back = expert_rows(arrived, own, e)
        grad_in[e] = dot(slot_in, acts[mine, hidden_width:], 0, 0).astype(NARROW)
        grad_out[e] = dot(acts[mine, :hidden_width], back, 0, 0).astype(NARROW)


def joined_results(planes, own, arrived, both):
    parts, half = arrived.shape[0] // planes, arrived.shape[2] // 2
    found = []
    for y in range(planes):
        total = arrived[y * parts].astype(WIDE)
        for t in range(1, parts):
            total += arrived[y * parts + t].astype(WIDE)
        found.append(total.astype(NARROW))
    found = jnp.concatenate(found)
    found = jnp.concatenate([found[:, :half], found[:, half:]])
    rows = found.shape[0]
    unit = 2 * planes * own
    both[...] = dot(turned(rows, unit, rows // unit, 1), found).astype(NARROW)


def dotted_rows(planes, own, arrived, exact, sent, column):
    slots, half = exact.shape
    unit = planes * own
    home = dot(turned(2 * slots, slots // unit, 2, unit), arrived[...])
    part = jnp.sum(exact[...] * home[slots:], axis=1, keepdims=True)
    column[...] = as_lanes([part])
    sent[: 2 * slots, :] = home.astype(NARROW)
    sent[2 * slots :, :] = as_lines(pieces(part, 3), half).astype(NARROW)


def softmax_grads(
    planes, cores, own, here, column, there, gathered, scores, stats, ordered, left, right, router
):
    slots = scores.shape[0]
    tokens, cotangent = image_tokens(gathered)
    lower = lax.axis_index("y_lo") == 0
    mine, other = here[: 2 * slots, :], there[: 2 * slots, :]
    joined = jnp.concatenate(
        [jnp.where(lower, mine, other), jnp.where(lower, other, mine)], axis=1
    )
    slot_out, grad_in = joined[:slots], joined[slots:]
    rest = as_columns(there[2 * slots :, :].astype(WIDE), slots)
    column_dot = column[:, 0:1] + (rest[:, 0:1] + rest[:, 1:2] + rest[:, 2:3])
    logits = scores[...]
    dispatch = jnp.exp(logits - stats[:, 0:1]) / stats[:, 1:2]
    combine = combine_of(logits)
    grad_combine = dot(slot_out, cotangent, 1, 1)
    grad_dispatch = dot(grad_in, tokens, 1, 1)
    row_dot = jnp.sum(grad_combine * combine, axis=0, keepdims=True)
    grad_logits = (
        combine * (grad_combine - row_dot) + dispatch * (grad_dispatch - column_dot)
    ).astype(NARROW)
    by_slot = dot(turned(slots, cores, planes, own), grad_logits).astype(NARROW)
    by_slot = dot(by_slot, tokens)
    count, high, wide = router.shape
    across = by_slot.shape[1] // wide
    for k in range(count):
        down, over = k // across * high, k % across * wide
        router[k] = by_slot[down : down + high, over : over + wide].astype(NARROW)
    left[:slots, :] = dispatch.astype(NARROW)
    left[slots:, :] = grad_logits
    right[:slots, :] = grad_in
    right[slots:, :] = ordered[...]


def token_grads(left, right, *refs):
    sent, found = refs[:-1], refs[-1]
    count, seq = found.shape[0], found.shape[1]
    grads = dot(left[...], right[...], 0, 0)
    for k in range(count):
        found[k] = grads[k * seq : (k + 1) * seq]
    here = lax.axis_index("x")
    for k in range(count):
        sent[k][...] = found[jnp.bitwise_xor(here, k)].astype(NARROW)


def placed_tokens(*refs):
    arrived, grad_tokens = refs[:-1], refs[-1]
    here = lax.axis_index("x")
    for k, block in enumerate(arrived):
        grad_tokens[jnp.bitwise_xor(here, k)] = block[...]


def summed_copies(arrived, sent):
    total = arrived[0].astype(WIDE)
    for t in range(1, arrived.shape[0]):
        total += arrived[t].astype(WIDE)
    for t in range(sent.shape[0]):
        sent[t] = total.astype(sent.dtype)


def placed(arrived, router):
    count, high, wide = arrived.shape
    across = router.shape[1] // wide
    for k in range(count):
        down, right = k // across * high, k % across * wide
        router[down : down + high, right : right + wide] = arrived[k].astype(router.dtype)


def local(body, outs, flops, *args, limit=12, scratch=()):
    moved = sum(a.size * a.dtype.itemsize for a in (*args, *outs))
    return pl.pallas_call(
        body,
        out_shape=outs,
        in_specs=[pl.BlockSpec(memory_space=pltpu.VMEM)] * len(args),
        out_specs=tuple([pl.BlockSpec(memory_space=pltpu.VMEM)] * len(outs)),
        scratch_shapes=scratch,
        cost_estimate=pl.CostEstimate(flops=flops, bytes_accessed=moved, transcendentals=0),
        compiler_params=pltpu.CompilerParams(vmem_limit_bytes=limit << 20),
    )(*args)


def shaped(shape, dtype=NARROW):
    return jax.ShapeDtypeStruct(shape, dtype)


def exchanged(blocks, axis):
    return lax.all_to_all(blocks, axis, split_axis=0, concat_axis=0, tiled=True)


def from_partner(block, axis, k):
    return lax.ppermute(block, axis, [(i, i ^ k) for i in range(lax.axis_size(axis))])


def on_device(tokens, cotangent, dispatch_weight, w_in, w_out):
    images, seq, width = tokens.shape
    slots = dispatch_weight.shape[1]
    own, hidden_width = w_in.shape[0], w_in.shape[2]
    planes, cores = lax.axis_size("y_hi"), lax.axis_size("core")
    plane, column = lax.axis_size(PLANE), lax.axis_size(COLUMN)
    half, count = width // 2, images * seq
    unit = planes * own
    rows = own * images * lax.axis_size(DP)

    both = jnp.concatenate([tokens, cotangent], axis=1)
    gathered = exchanged(both, "x")
    sent, kept, scores, stats, ordered = local(
        functools.partial(slot_rows, planes, cores, own),
        (
            shaped((2 * slots + EXTRA, half)),
            shaped((2 * slots, half), WIDE),
            shaped((slots, count), WIDE),
            shaped((slots, LANES), WIDE),
            shaped((slots, width)),
        ),
        8 * slots * count * width,
        gathered,
        dispatch_weight.T,
    )
    both, exact, stats = local(
        functools.partial(joined_rows, planes, own),
        (shaped((2 * slots, half)), shaped((slots, half), WIDE), shaped((slots, LANES), WIDE)),
        4 * slots * slots * width,
        from_partner(sent, "y_lo", 1),
        kept,
        stats,
    )
    arrived = exchanged(both.reshape(column, 2 * unit, half), COLUMN).reshape(2 * slots, half)
    high = own * column
    (sent,) = local(
        functools.partial(sorted_copies, planes, own),
        (shaped((plane, high, width)),),
        4 * slots * slots * width,
        arrived,
    )
    arrived = exchanged(sent, PLANE)
    sent, acts = local(
        experts,
        (shaped((plane, high, width)), shaped((rows, 2 * hidden_width))),
        8 * rows * width * hidden_width,
        arrived,
        w_in,
        w_out,
    )
    back = exchanged(sent, PLANE)
    grad_w_in, grad_w_out = local(
        weight_grads,
        (shaped(w_in.shape), shaped(w_out.shape)),
        4 * rows * width * hidden_width,
        arrived,
        acts,
    )
    (both,) = local(
        functools.partial(joined_results, planes, own),
        (shaped((2 * slots, half)),),
        4 * slots * slots * width,
        back,
    )
    arrived = exchanged(both.reshape(column, 2 * unit, half), COLUMN).reshape(2 * slots, half)
    sent, part = local(
        functools.partial(dotted_rows, planes, own),
        (shaped((2 * slots + EXTRA, half)), shaped((slots, LANES), WIDE)),
        4 * slots * slots * width,
        arrived,
        exact,
    )
    across = width // LANES
    tall = slots * across // plane
    left, right, router = local(
        functools.partial(softmax_grads, planes, cores, own),
        (
            shaped((2 * slots, count)),
            shaped((2 * slots, width)),
            shaped((plane, tall, LANES)),
        ),
        6 * slots * count * width,
        sent,
        part,
        from_partner(sent, "y_lo", 1),
        gathered,
        scores,
        stats,
        ordered,
    )
    blocks = local(
        token_grads,
        tuple([shaped((seq, width))] * images),
        4 * slots * count * width,
        left,
        right,
        scratch=(pltpu.VMEM((images, seq, width), WIDE),),
    )
    blocks = [blocks[0]] + [from_partner(blocks[k], "x", k) for k in range(1, images)]
    (grad_tokens,) = local(
        placed_tokens, (shaped((images, seq, width)),), count * width, *blocks
    )
    (router,) = local(
        summed_copies,
        (shaped((column, tall, LANES)),),
        slots * width,
        exchanged(router, PLANE),
    )
    (router,) = local(
        summed_copies,
        (shaped((plane, tall, LANES)),),
        slots * width,
        exchanged(router, COLUMN),
    )
    (router,) = local(
        placed, (shaped((slots, width), WIDE),), slots * width, exchanged(router, PLANE)
    )
    return (grad_tokens, router.T, grad_w_in, grad_w_out)


def solution(mesh):
    groups, parts = mesh.devices.shape
    fine = Mesh(
        mesh.devices.reshape(groups // 4, 2, 2, parts // 2, 2),
        ("z", "y_hi", "core", "x", "y_lo"),
    )
    return jax.shard_map(
        on_device,
        mesh=fine,
        in_specs=(
            P(DP, TENSOR, None),
            P(DP, TENSOR, None),
            P(),
            P(DP, None, TENSOR),
            P(DP, TENSOR, None),
        ),
        out_specs=(P(DP, TENSOR, None), P(), P(DP, None, TENSOR), P(DP, TENSOR, None)),
        check_vma=False,
    )
```

```python
import functools

import jax
import jax.numpy as jnp
from jax import lax
from jax.experimental import pallas as pl
from jax.experimental.pallas import tpu as pltpu
from jax.sharding import Mesh
from jax.sharding import PartitionSpec as P

NARROW = jnp.bfloat16
WIDE = jnp.float32
LANES = 128
EXTRA = 8
DP = ("z", "y_hi", "core")
TENSOR = ("x", "y_lo")
PLANE = ("y_hi", "x", "y_lo")
COLUMN = ("z", "core")


def dot(a, b, over_a=1, over_b=0):
    return lax.dot_general(a, b, (((over_a,), (over_b,)), ((), ())), preferred_element_type=WIDE)


def iota(shape, dim):
    return lax.broadcasted_iota(jnp.int32, shape, dim)


def pieces(x, count):
    found = []
    for _ in range(count):
        piece = x.astype(NARROW).astype(WIDE)
        found.append(piece)
        x = x - piece
    return found


def as_lanes(columns):
    rows = columns[0].shape[0]
    lane = iota((rows, LANES), 1)
    found = jnp.zeros((rows, LANES), WIDE)
    for k, column in enumerate(columns):
        found = jnp.where(lane == k, column, found)
    return found


def as_lines(columns, width):
    square = as_lanes(columns)
    square = jnp.concatenate([square, jnp.zeros((LANES - square.shape[0], LANES), WIDE)])
    lines = square.T[:EXTRA]
    return jnp.concatenate([lines, jnp.zeros((EXTRA, width - LANES), WIDE)], axis=1)


def as_columns(lines, rows):
    lines = lines[:, :LANES]
    return jnp.concatenate([lines, jnp.zeros((LANES - EXTRA, LANES), WIDE)]).T[:rows]


def selection(size, source):
    return (iota((size, size), 1) == source(iota((size, size), 0))).astype(NARROW)


def turned(size, outer, inner, unit):
    def source(row):
        a = row // unit % outer
        b = row // (unit * outer) % inner
        rest = row // (unit * outer * inner)
        return ((rest * outer + a) * inner + b) * unit + row % unit

    return selection(size, source)


def combine_of(scores):
    weight = jnp.exp(scores - jnp.max(scores, axis=0, keepdims=True))
    return weight / jnp.sum(weight, axis=0, keepdims=True)


def sorted_blocks(both, *sent):
    here = lax.axis_index("x")
    for k, block in enumerate(sent):
        block[...] = both[jnp.bitwise_xor(here, k)]


def image_tokens(blocks):
    seq = blocks[0].shape[0] // 2
    return tuple(
        jnp.concatenate([block[f * seq : (f + 1) * seq, :] for block in blocks]) for f in range(2)
    )


def slot_rows(planes, cores, own, *refs):
    router, sent, kept, scores, stats, ordered = refs[-6:]
    gathered = refs[:-6]
    slots, width = router.shape
    half = width // 2
    tokens, cotangent = image_tokens(gathered)
    ordered[...] = dot(turned(slots, planes, cores, own), router[...]).astype(NARROW)
    logits = dot(ordered[...], tokens, 1, 1)
    scores[...] = logits
    high, low = pieces(jnp.max(logits, axis=1, keepdims=True), 2)
    weight = jnp.exp(logits - (high + low))
    total = jnp.sum(weight, axis=1, keepdims=True)
    stats[...] = as_lanes([high + low, total])
    first, second = (piece.astype(NARROW) for piece in pieces(weight, 2))
    part_in = dot(first, tokens) + dot(second, tokens)
    part_back = dot(combine_of(logits).astype(NARROW), cotangent)
    lower = lax.axis_index("core") == 0
    for k, part in enumerate((part_in, part_back)):
        mine = slice(k * slots, (k + 1) * slots)
        kept[mine, :] = jnp.where(lower, part[:, :half], part[:, half:])
        sent[mine, :] = jnp.where(lower, part[:, half:], part[:, :half]).astype(NARROW)
    sent[2 * slots :, :] = as_lines([high, low, *pieces(total, 2)], half).astype(NARROW)


def joined_rows(planes, own, arrived, kept, local_stats, both, exact, stats):
    slots = exact.shape[0]
    there = as_columns(arrived[2 * slots :, :].astype(WIDE), slots)
    top_here, total_here = local_stats[:, 0:1], local_stats[:, 1:2]
    top_there, total_there = there[:, 0:1] + there[:, 1:2], there[:, 2:3] + there[:, 3:4]
    top = jnp.maximum(top_here, top_there)
    here, there = jnp.exp(top_here - top), jnp.exp(top_there - top)
    total = here * total_here + there * total_there
    stats[...] = as_lanes([top, total])
    slot_part = kept[:slots, :] * (here / total) + arrived[:slots, :].astype(WIDE) * (there / total)
    back_part = kept[slots:, :] + arrived[slots : 2 * slots, :].astype(WIDE)
    exact[...] = slot_part
    narrow = jnp.concatenate([slot_part, back_part]).astype(NARROW)
    unit = planes * own
    both[...] = dot(turned(2 * slots, 2, slots // unit, unit), narrow).astype(NARROW)


def sorted_copies(planes, arrived, sent):
    rows = arrived.shape[0]
    high = sent.shape[1]
    ordered = dot(turned(rows, rows // 16, 16, 1), arrived[...]).astype(NARROW)
    part = planes * high
    ordered = jnp.concatenate(
        [ordered[j * part : (j + 1) * part] for j in (0, 2, 1, 3)], axis=1
    )
    for k in range(sent.shape[0]):
        first = k // (sent.shape[0] // planes) * high
        sent[k] = ordered[first : first + high]


def expert_rows(arrived, own, e):
    each = arrived.shape[1] // own
    width = arrived.shape[2] // 2
    return tuple(
        jnp.concatenate(
            [
                arrived[j, e * each : (e + 1) * each, k * width : (k + 1) * width]
                for j in range(arrived.shape[0])
            ]
        )
        for k in range(2)
    )


def experts(arrived, w_in, w_out, sent, acts):
    own, hidden_width = w_in.shape[0], w_in.shape[2]
    each, high, width = acts.shape[0] // own, arrived.shape[1] // own, arrived.shape[2] // 2
    root = (2.0 / jnp.pi) ** 0.5
    for e in range(own):
        mine = slice(e * each, (e + 1) * each)
        there = slice(e * high, (e + 1) * high)
        slot_in, back = expert_rows(arrived, own, e)
        v = dot(slot_in, w_in[e])
        grad_hidden = dot(back, w_out[e], 1, 1)
        t = jnp.tanh(root * (v + 0.044715 * (v * v * v)))
        upper = 0.5 * (1.0 + t)
        low = (v * upper).astype(NARROW)
        slope = upper + 0.5 * v * (1.0 - t * t) * (root * (1.0 + 3 * 0.044715 * (v * v)))
        grad_low = (slope * grad_hidden).astype(NARROW)
        acts[mine, :hidden_width] = low
        acts[mine, hidden_width:] = grad_low
        slot_out = dot(low, w_out[e]).astype(NARROW)
        grad_in = dot(grad_low, w_in[e], 1, 1).astype(NARROW)
        for k in range(sent.shape[0]):
            sent[k, there, :width] = slot_out[k * high : (k + 1) * high]
            sent[k, there, width:] = grad_in[k * high : (k + 1) * high]


def weight_grads(arrived, acts, grad_in, grad_out):
    own, hidden_width = grad_in.shape[0], grad_in.shape[2]
    each = acts.shape[0] // own
    for e in range(own):
        mine = slice(e * each, (e + 1) * each)
        slot_in, back = expert_rows(arrived, own, e)
        grad_in[e] = dot(slot_in, acts[mine, hidden_width:], 0, 0).astype(NARROW)
        grad_out[e] = dot(acts[mine, :hidden_width], back, 0, 0).astype(NARROW)


def joined_results(planes, arrived, both):
    parts, half = arrived.shape[0] // planes, both.shape[1]
    found = []
    for y in range(planes):
        total = arrived[y * parts].astype(WIDE)
        for t in range(1, parts):
            total += arrived[y * parts + t].astype(WIDE)
        found.append(total.astype(NARROW))
    found = jnp.concatenate(found)
    found = jnp.concatenate([found[:, j * half : (j + 1) * half] for j in (0, 2, 1, 3)])
    rows = found.shape[0]
    both[...] = dot(turned(rows, 16, rows // 16, 1), found).astype(NARROW)


def dotted_rows(planes, own, arrived, exact, sent, column):
    slots, half = exact.shape
    unit = planes * own
    home = dot(turned(2 * slots, slots // unit, 2, unit), arrived[...])
    part = jnp.sum(exact[...] * home[slots:], axis=1, keepdims=True)
    column[...] = as_lanes([part])
    sent[: 2 * slots, :] = home.astype(NARROW)
    sent[2 * slots :, :] = as_lines(pieces(part, 3), half).astype(NARROW)


def softmax_grads(planes, cores, own, *refs):
    here, column, there, scores, stats, ordered, left, right, router = refs[-9:]
    gathered = refs[:-9]
    slots = scores.shape[0]
    tokens, cotangent = image_tokens(gathered)
    lower = lax.axis_index("core") == 0
    mine, other = here[: 2 * slots, :], there[: 2 * slots, :]
    joined = jnp.concatenate(
        [jnp.where(lower, mine, other), jnp.where(lower, other, mine)], axis=1
    )
    slot_out, grad_in = joined[:slots], joined[slots:]
    rest = as_columns(there[2 * slots :, :].astype(WIDE), slots)
    column_dot = column[:, 0:1] + (rest[:, 0:1] + rest[:, 1:2] + rest[:, 2:3])
    logits = scores[...]
    dispatch = jnp.exp(logits - stats[:, 0:1]) / stats[:, 1:2]
    combine = combine_of(logits)
    grad_combine = dot(slot_out, cotangent, 1, 1)
    grad_dispatch = dot(grad_in, tokens, 1, 1)
    row_dot = jnp.sum(grad_combine * combine, axis=0, keepdims=True)
    grad_logits = (
        combine * (grad_combine - row_dot) + dispatch * (grad_dispatch - column_dot)
    ).astype(NARROW)
    by_slot = dot(turned(slots, cores, planes, own), grad_logits).astype(NARROW)
    by_slot = dot(by_slot, tokens)
    count, high, wide = router.shape
    across = by_slot.shape[1] // wide
    for k in range(count):
        down, over = k // across * high, k % across * wide
        router[k] = by_slot[down : down + high, over : over + wide].astype(NARROW)
    left[:slots, :] = dispatch.astype(NARROW)
    left[slots:, :] = grad_logits
    right[:slots, :] = grad_in
    right[slots:, :] = ordered[...]


def token_grads(left, right, *sent):
    seq = sent[0].shape[0]
    grads = dot(left[...], right[...], 0, 0)
    for k, block in enumerate(sent):
        block[...] = grads[k * seq : (k + 1) * seq].astype(NARROW)


def placed_tokens(*refs):
    arrived, grad_tokens = refs[:-1], refs[-1]
    here = lax.axis_index("x")
    for k, block in enumerate(arrived):
        grad_tokens[jnp.bitwise_xor(here, k)] = block[...]


def summed_copies(arrived, sent):
    total = arrived[0].astype(WIDE)
    for t in range(1, arrived.shape[0]):
        total += arrived[t].astype(WIDE)
    for t in range(sent.shape[0]):
        sent[t] = total.astype(sent.dtype)


def placed(arrived, router):
    count, high, wide = arrived.shape
    across = router.shape[1] // wide
    for k in range(count):
        down, right = k // across * high, k % across * wide
        router[down : down + high, right : right + wide] = arrived[k].astype(router.dtype)


def local(body, outs, flops, *args, limit=12):
    moved = sum(a.size * a.dtype.itemsize for a in (*args, *outs))
    return pl.pallas_call(
        body,
        out_shape=outs,
        in_specs=[pl.BlockSpec(memory_space=pltpu.VMEM)] * len(args),
        out_specs=tuple([pl.BlockSpec(memory_space=pltpu.VMEM)] * len(outs)),
        cost_estimate=pl.CostEstimate(flops=flops, bytes_accessed=moved, transcendentals=0),
        compiler_params=pltpu.CompilerParams(vmem_limit_bytes=limit << 20),
    )(*args)


def shaped(shape, dtype=NARROW):
    return jax.ShapeDtypeStruct(shape, dtype)


def exchanged(blocks, axis):
    return lax.all_to_all(blocks, axis, split_axis=0, concat_axis=0, tiled=True)


def from_partner(block):
    return lax.ppermute(block, "core", [(0, 1), (1, 0)])


def moved(block, k):
    axes = ("core", "x", "y_lo")
    across = lax.axis_size("x")
    pairs = []
    for core in range(2):
        for x in range(across):
            for low in range(2):
                source = (core * across + x) * 2 + low
                pairs.append((source, (low * across + (x ^ k)) * 2 + core))
    return lax.ppermute(block, axes, pairs)


def on_device(tokens, cotangent, dispatch_weight, w_in, w_out):
    images, seq, width = tokens.shape
    slots = dispatch_weight.shape[1]
    own, hidden_width = w_in.shape[0], w_in.shape[2]
    planes, cores = lax.axis_size("y_hi"), lax.axis_size("core")
    plane, column = lax.axis_size(PLANE), lax.axis_size(COLUMN)
    half, count = width // 2, images * seq
    unit = planes * own
    rows = own * images * lax.axis_size(DP)

    both = jnp.concatenate([tokens, cotangent], axis=1)
    blocks = local(
        sorted_blocks, tuple([shaped((2 * seq, width))] * images), count * width, both
    )
    gathered = [moved(block, k) for k, block in enumerate(blocks)]
    sent, kept, scores, stats, ordered = local(
        functools.partial(slot_rows, planes, cores, own),
        (
            shaped((2 * slots + EXTRA, half)),
            shaped((2 * slots, half), WIDE),
            shaped((slots, count), WIDE),
            shaped((slots, LANES), WIDE),
            shaped((slots, width)),
        ),
        8 * slots * count * width,
        *gathered,
        dispatch_weight.T,
    )
    both, exact, stats = local(
        functools.partial(joined_rows, planes, own),
        (shaped((2 * slots, half)), shaped((slots, half), WIDE), shaped((slots, LANES), WIDE)),
        4 * slots * slots * width,
        from_partner(sent),
        kept,
        stats,
    )
    arrived = exchanged(both.reshape(column, 2 * unit, half), COLUMN).reshape(2 * slots, half)
    high = own * lax.axis_size("z")
    (sent,) = local(
        functools.partial(sorted_copies, planes),
        (shaped((plane, high, 2 * width)),),
        4 * slots * slots * width,
        arrived,
    )
    arrived = exchanged(sent, PLANE)
    sent, acts = local(
        experts,
        (shaped((plane, high, 2 * width)), shaped((rows, 2 * hidden_width))),
        8 * rows * width * hidden_width,
        arrived,
        w_in,
        w_out,
    )
    back = exchanged(sent, PLANE)
    grad_w_in, grad_w_out = local(
        weight_grads,
        (shaped(w_in.shape), shaped(w_out.shape)),
        4 * rows * width * hidden_width,
        arrived,
        acts,
    )
    (both,) = local(
        functools.partial(joined_results, planes),
        (shaped((2 * slots, half)),),
        4 * slots * slots * width,
        back,
    )
    arrived = exchanged(both.reshape(column, 2 * unit, half), COLUMN).reshape(2 * slots, half)
    sent, part = local(
        functools.partial(dotted_rows, planes, own),
        (shaped((2 * slots + EXTRA, half)), shaped((slots, LANES), WIDE)),
        4 * slots * slots * width,
        arrived,
        exact,
    )
    across = width // LANES
    tall = slots * across // plane
    left, right, router = local(
        functools.partial(softmax_grads, planes, cores, own),
        (
            shaped((2 * slots, count)),
            shaped((2 * slots, width)),
            shaped((plane, tall, LANES)),
        ),
        6 * slots * count * width,
        *gathered,
        sent,
        part,
        from_partner(sent),
        scores,
        stats,
        ordered,
    )
    blocks = local(
        token_grads,
        tuple([shaped((seq, width))] * images),
        4 * slots * count * width,
        left,
        right,
    )
    blocks = [moved(block, k) for k, block in enumerate(blocks)]
    (grad_tokens,) = local(
        placed_tokens, (shaped((images, seq, width)),), count * width, *blocks
    )
    (router,) = local(
        summed_copies,
        (shaped((column, tall, LANES)),),
        slots * width,
        exchanged(router, PLANE),
    )
    (router,) = local(
        summed_copies,
        (shaped((plane, tall, LANES)),),
        slots * width,
        exchanged(router, COLUMN),
    )
    (router,) = local(
        placed, (shaped((slots, width), WIDE),), slots * width, exchanged(router, PLANE)
    )
    return (grad_tokens, router.T, grad_w_in, grad_w_out)


def solution(mesh):
    groups, parts = mesh.devices.shape
    fine = Mesh(
        mesh.devices.reshape(groups // 4, 2, 2, parts // 2, 2),
        ("z", "y_hi", "core", "x", "y_lo"),
    )
    return jax.shard_map(
        on_device,
        mesh=fine,
        in_specs=(
            P(DP, TENSOR, None),
            P(DP, TENSOR, None),
            P(),
            P(DP, None, TENSOR),
            P(DP, TENSOR, None),
        ),
        out_specs=(P(DP, TENSOR, None), P(), P(DP, None, TENSOR), P(DP, TENSOR, None)),
        check_vma=False,
    )
```

```python
import functools

import jax
import jax.numpy as jnp
from jax import lax
from jax.experimental import pallas as pl
from jax.experimental.pallas import tpu as pltpu
from jax.sharding import Mesh
from jax.sharding import PartitionSpec as P

NARROW = jnp.bfloat16
WIDE = jnp.float32
LANES = 128
EXTRA = 8
DP = ("z", "y_hi", "core")
TENSOR = ("x", "y_lo")
PLANE = ("y_hi", "x", "y_lo")
COLUMN = ("z", "core")


def dot(a, b, over_a=1, over_b=0):
    return lax.dot_general(a, b, (((over_a,), (over_b,)), ((), ())), preferred_element_type=WIDE)


def iota(shape, dim):
    return lax.broadcasted_iota(jnp.int32, shape, dim)


def pieces(x, count):
    found = []
    for _ in range(count):
        piece = x.astype(NARROW).astype(WIDE)
        found.append(piece)
        x = x - piece
    return found


def as_lanes(columns):
    rows = columns[0].shape[0]
    lane = iota((rows, LANES), 1)
    found = jnp.zeros((rows, LANES), WIDE)
    for k, column in enumerate(columns):
        found = jnp.where(lane == k, column, found)
    return found


def as_lines(columns, width):
    square = as_lanes(columns)
    square = jnp.concatenate([square, jnp.zeros((LANES - square.shape[0], LANES), WIDE)])
    lines = square.T[:EXTRA]
    return jnp.concatenate([lines, jnp.zeros((EXTRA, width - LANES), WIDE)], axis=1)


def as_columns(lines, rows):
    lines = lines[:, :LANES]
    return jnp.concatenate([lines, jnp.zeros((LANES - EXTRA, LANES), WIDE)]).T[:rows]


def selection(size, source):
    return (iota((size, size), 1) == source(iota((size, size), 0))).astype(NARROW)


def turned(size, outer, inner, unit):
    def source(row):
        a = row // unit % outer
        b = row // (unit * outer) % inner
        rest = row // (unit * outer * inner)
        return ((rest * outer + a) * inner + b) * unit + row % unit

    return selection(size, source)


def combine_of(scores):
    weight = jnp.exp(scores - jnp.max(scores, axis=0, keepdims=True))
    return weight / jnp.sum(weight, axis=0, keepdims=True)


def sorted_blocks(both, *sent):
    here = lax.axis_index("x")
    for k, block in enumerate(sent):
        block[...] = both[jnp.bitwise_xor(here, k)]


def image_tokens(blocks):
    seq = blocks[0].shape[0] // 2
    return tuple(
        jnp.concatenate([block[f * seq : (f + 1) * seq, :] for block in blocks]) for f in range(2)
    )


def own_first(mine, other):
    lower = lax.axis_index("core") == 0
    return jnp.concatenate([jnp.where(lower, mine, other), jnp.where(lower, other, mine)])


def cores_rows(rows):
    lower = lax.axis_index("core") == 0
    first, second = rows[: rows.shape[0] // 2], rows[rows.shape[0] // 2 :]
    return jnp.where(lower, first, second), jnp.where(lower, second, first)


def slot_rows(cores, own, *refs):
    router, sent, kept, scores, stats, ordered = refs[-6:]
    gathered = refs[:-6]
    slots, width = router.shape
    half = slots // 2
    tokens, cotangent = image_tokens(gathered)
    order = turned(slots, slots // (cores * own), cores, own)
    ordered[...] = dot(order, router[...]).astype(NARROW)
    logits = dot(ordered[...], tokens, 1, 1)
    scores[...] = logits
    high, low = pieces(jnp.max(logits, axis=1, keepdims=True), 2)
    weight = jnp.exp(logits - (high + low))
    total = jnp.sum(weight, axis=1, keepdims=True)
    stats[...] = as_lanes([high + low, total])
    first, second = (piece.astype(NARROW) for piece in pieces(weight, 2))
    part_in = dot(first, tokens) + dot(second, tokens)
    part_back = dot(combine_of(logits).astype(NARROW), cotangent)
    for k, part in enumerate((part_in, part_back)):
        place = slice(k * half, (k + 1) * half)
        mine, other = cores_rows(part)
        kept[place, :] = mine
        sent[place, :] = other.astype(NARROW)
    sent[slots:, :] = as_lines([high, low, *pieces(total, 2)], width).astype(NARROW)


def joined_rows(unit, arrived, kept, local_stats, both, exact, stats):
    half = exact.shape[0]
    slots = 2 * half
    there = as_columns(arrived[slots:, :].astype(WIDE), slots)
    top_here, total_here = local_stats[:, 0:1], local_stats[:, 1:2]
    top_there, total_there = there[:, 0:1] + there[:, 1:2], there[:, 2:3] + there[:, 3:4]
    top = jnp.maximum(top_here, top_there)
    here, there = jnp.exp(top_here - top), jnp.exp(top_there - top)
    total = here * total_here + there * total_there
    stats[...] = as_lanes([top, total])
    scale_here, _ = cores_rows(here / total)
    scale_there, _ = cores_rows(there / total)
    slot_part = kept[:half, :] * scale_here + arrived[:half, :].astype(WIDE) * scale_there
    back_part = kept[half:, :] + arrived[half:slots, :].astype(WIDE)
    exact[...] = slot_part
    narrow = jnp.concatenate([slot_part, back_part]).astype(NARROW)
    both[...] = dot(turned(slots, 2, half // unit, unit), narrow).astype(NARROW)


def sorted_copies(planes, unit, arrived, sent):
    rows, high = arrived.shape[0], sent.shape[1]
    ordered = dot(turned(rows, rows // (2 * unit), 2 * unit, 1), arrived[...]).astype(NARROW)
    ordered = jnp.concatenate([ordered[: rows // 2], ordered[rows // 2 :]], axis=1)
    for k in range(sent.shape[0]):
        first = k // (sent.shape[0] // planes) * high
        sent[k] = ordered[first : first + high]


def expert_rows(arrived, own, e):
    each = arrived.shape[1] // own
    width = arrived.shape[2] // 2
    return tuple(
        jnp.concatenate(
            [
                arrived[j, e * each : (e + 1) * each, k * width : (k + 1) * width]
                for j in range(arrived.shape[0])
            ]
        )
        for k in range(2)
    )


def experts(arrived, w_in, w_out, sent, acts):
    own, hidden_width = w_in.shape[0], w_in.shape[2]
    each, high, width = acts.shape[0] // own, arrived.shape[1] // own, arrived.shape[2] // 2
    root = (2.0 / jnp.pi) ** 0.5
    for e in range(own):
        mine = slice(e * each, (e + 1) * each)
        there = slice(e * high, (e + 1) * high)
        slot_in, back = expert_rows(arrived, own, e)
        v = dot(slot_in, w_in[e])
        grad_hidden = dot(back, w_out[e], 1, 1)
        t = jnp.tanh(root * (v + 0.044715 * (v * v * v)))
        upper = 0.5 * (1.0 + t)
        low = (v * upper).astype(NARROW)
        slope = upper + 0.5 * v * (1.0 - t * t) * (root * (1.0 + 3 * 0.044715 * (v * v)))
        grad_low = (slope * grad_hidden).astype(NARROW)
        acts[mine, :hidden_width] = low
        acts[mine, hidden_width:] = grad_low
        slot_out = dot(low, w_out[e]).astype(NARROW)
        grad_in = dot(grad_low, w_in[e], 1, 1).astype(NARROW)
        for k in range(sent.shape[0]):
            sent[k, there, :width] = slot_out[k * high : (k + 1) * high]
            sent[k, there, width:] = grad_in[k * high : (k + 1) * high]


def weight_grads(arrived, acts, grad_in, grad_out):
    own, hidden_width = grad_in.shape[0], grad_in.shape[2]
    each = acts.shape[0] // own
    for e in range(own):
        mine = slice(e * each, (e + 1) * each)
        slot_in, back = expert_rows(arrived, own, e)
        grad_in[e] = dot(slot_in, acts[mine, hidden_width:], 0, 0).astype(NARROW)
        grad_out[e] = dot(acts[mine, :hidden_width], back, 0, 0).astype(NARROW)


def joined_results(planes, unit, arrived, both):
    parts, width = arrived.shape[0] // planes, both.shape[1]
    found = []
    for y in range(planes):
        total = arrived[y * parts].astype(WIDE)
        for t in range(1, parts):
            total += arrived[y * parts + t].astype(WIDE)
        found.append(total.astype(NARROW))
    found = jnp.concatenate(found)
    found = jnp.concatenate([found[:, :width], found[:, width:]])
    rows = found.shape[0]
    both[...] = dot(turned(rows, 2 * unit, rows // (2 * unit), 1), found).astype(NARROW)


def dotted_rows(unit, arrived, exact, sent, column):
    half, width = exact.shape
    home = dot(turned(2 * half, half // unit, 2, unit), arrived[...])
    part = jnp.sum(exact[...] * home[half:], axis=1, keepdims=True)
    column[...] = as_lanes([part])
    sent[: 2 * half, :] = home.astype(NARROW)
    sent[2 * half :, :] = as_lines(pieces(part, 3), width).astype(NARROW)


def softmax_grads(cores, own, *refs):
    here, column, there, scores, stats, ordered, left, right, router = refs[-9:]
    gathered = refs[:-9]
    slots = scores.shape[0]
    half = slots // 2
    tokens, cotangent = image_tokens(gathered)
    slot_out = own_first(here[:half, :], there[:half, :])
    grad_in = own_first(here[half:slots, :], there[half:slots, :])
    rest = as_columns(there[slots:, :].astype(WIDE), half)
    column_dot = own_first(column[:, 0:1], rest[:, 0:1] + rest[:, 1:2] + rest[:, 2:3])
    logits = scores[...]
    dispatch = jnp.exp(logits - stats[:, 0:1]) / stats[:, 1:2]
    combine = combine_of(logits)
    grad_combine = dot(slot_out, cotangent, 1, 1)
    grad_dispatch = dot(grad_in, tokens, 1, 1)
    row_dot = jnp.sum(grad_combine * combine, axis=0, keepdims=True)
    grad_logits = (
        combine * (grad_combine - row_dot) + dispatch * (grad_dispatch - column_dot)
    ).astype(NARROW)
    order = turned(slots, cores, slots // (cores * own), own)
    by_slot = dot(dot(order, grad_logits).astype(NARROW), tokens)
    count, high, wide = router.shape
    across = by_slot.shape[1] // wide
    for k in range(count):
        down, over = k // across * high, k % across * wide
        router[k] = by_slot[down : down + high, over : over + wide].astype(NARROW)
    left[:slots, :] = dispatch.astype(NARROW)
    left[slots:, :] = grad_logits
    right[:slots, :] = grad_in
    right[slots:, :] = ordered[...]


def token_grads(left, right, *sent):
    seq = sent[0].shape[0]
    grads = dot(left[...], right[...], 0, 0)
    for k, block in enumerate(sent):
        block[...] = grads[k * seq : (k + 1) * seq].astype(NARROW)


def placed_tokens(*refs):
    arrived, grad_tokens = refs[:-1], refs[-1]
    here = lax.axis_index("x")
    for k, block in enumerate(arrived):
        grad_tokens[jnp.bitwise_xor(here, k)] = block[...]


def summed_copies(arrived, sent):
    total = arrived[0].astype(WIDE)
    for t in range(1, arrived.shape[0]):
        total += arrived[t].astype(WIDE)
    for t in range(sent.shape[0]):
        sent[t] = total.astype(sent.dtype)


def placed(arrived, router):
    count, high, wide = arrived.shape
    across = router.shape[1] // wide
    for k in range(count):
        down, right = k // across * high, k % across * wide
        router[down : down + high, right : right + wide] = arrived[k].astype(router.dtype)


def local(body, outs, flops, *args, limit=12):
    moved = sum(a.size * a.dtype.itemsize for a in (*args, *outs))
    return pl.pallas_call(
        body,
        out_shape=outs,
        in_specs=[pl.BlockSpec(memory_space=pltpu.VMEM)] * len(args),
        out_specs=tuple([pl.BlockSpec(memory_space=pltpu.VMEM)] * len(outs)),
        cost_estimate=pl.CostEstimate(flops=flops, bytes_accessed=moved, transcendentals=0),
        compiler_params=pltpu.CompilerParams(vmem_limit_bytes=limit << 20),
    )(*args)


def shaped(shape, dtype=NARROW):
    return jax.ShapeDtypeStruct(shape, dtype)


def exchanged(blocks, axis):
    return lax.all_to_all(blocks, axis, split_axis=0, concat_axis=0, tiled=True)


def from_partner(block):
    return lax.ppermute(block, "core", [(0, 1), (1, 0)])


def moved(block, k):
    axes = ("core", "x", "y_lo")
    across = lax.axis_size("x")
    pairs = []
    for core in range(2):
        for x in range(across):
            for low in range(2):
                source = (core * across + x) * 2 + low
                pairs.append((source, (low * across + (x ^ k)) * 2 + core))
    return lax.ppermute(block, axes, pairs)


def on_device(tokens, cotangent, dispatch_weight, w_in, w_out):
    images, seq, width = tokens.shape
    slots = dispatch_weight.shape[1]
    own, hidden_width = w_in.shape[0], w_in.shape[2]
    planes, cores = lax.axis_size("y_hi"), lax.axis_size("core")
    plane, column = lax.axis_size(PLANE), lax.axis_size(COLUMN)
    half, count, depth = slots // 2, images * seq, lax.axis_size("z")
    unit = planes * own
    rows = own * images * lax.axis_size(DP)

    both = jnp.concatenate([tokens, cotangent], axis=1)
    blocks = local(
        sorted_blocks, tuple([shaped((2 * seq, width))] * images), count * width, both
    )
    gathered = [moved(block, k) for k, block in enumerate(blocks)]
    sent, kept, scores, stats, ordered = local(
        functools.partial(slot_rows, cores, own),
        (
            shaped((slots + EXTRA, width)),
            shaped((slots, width), WIDE),
            shaped((slots, count), WIDE),
            shaped((slots, LANES), WIDE),
            shaped((slots, width)),
        ),
        8 * slots * count * width,
        *gathered,
        dispatch_weight.T,
    )
    both, exact, stats = local(
        functools.partial(joined_rows, unit),
        (shaped((slots, width)), shaped((half, width), WIDE), shaped((slots, LANES), WIDE)),
        4 * slots * slots * width,
        from_partner(sent),
        kept,
        stats,
    )
    arrived = exchanged(both.reshape(depth, 2 * unit, width), "z").reshape(slots, width)
    high = own * depth
    (sent,) = local(
        functools.partial(sorted_copies, planes, unit),
        (shaped((plane, high, 2 * width)),),
        4 * slots * slots * width,
        arrived,
    )
    arrived = exchanged(sent, PLANE)
    sent, acts = local(
        experts,
        (shaped((plane, high, 2 * width)), shaped((rows, 2 * hidden_width))),
        8 * rows * width * hidden_width,
        arrived,
        w_in,
        w_out,
    )
    back = exchanged(sent, PLANE)
    grad_w_in, grad_w_out = local(
        weight_grads,
        (shaped(w_in.shape), shaped(w_out.shape)),
        4 * rows * width * hidden_width,
        arrived,
        acts,
    )
    (both,) = local(
        functools.partial(joined_results, planes, unit),
        (shaped((slots, width)),),
        4 * slots * slots * width,
        back,
    )
    arrived = exchanged(both.reshape(depth, 2 * unit, width), "z").reshape(slots, width)
    sent, part = local(
        functools.partial(dotted_rows, unit),
        (shaped((slots + EXTRA, width)), shaped((half, LANES), WIDE)),
        4 * slots * slots * width,
        arrived,
        exact,
    )
    across = width // LANES
    tall = slots * across // plane
    left, right, router = local(
        functools.partial(softmax_grads, cores, own),
        (
            shaped((2 * slots, count)),
            shaped((2 * slots, width)),
            shaped((plane, tall, LANES)),
        ),
        6 * slots * count * width,
        *gathered,
        sent,
        part,
        from_partner(sent),
        scores,
        stats,
        ordered,
    )
    blocks = local(
        token_grads,
        tuple([shaped((seq, width))] * images),
        4 * slots * count * width,
        left,
        right,
    )
    blocks = [moved(block, k) for k, block in enumerate(blocks)]
    (grad_tokens,) = local(
        placed_tokens, (shaped((images, seq, width)),), count * width, *blocks
    )
    (router,) = local(
        summed_copies,
        (shaped((column, tall, LANES)),),
        slots * width,
        exchanged(router, PLANE),
    )
    (router,) = local(
        summed_copies,
        (shaped((plane, tall, LANES)),),
        slots * width,
        exchanged(router, COLUMN),
    )
    (router,) = local(
        placed, (shaped((slots, width), WIDE),), slots * width, exchanged(router, PLANE)
    )
    return (grad_tokens, router.T, grad_w_in, grad_w_out)


def solution(mesh):
    groups, parts = mesh.devices.shape
    fine = Mesh(
        mesh.devices.reshape(groups // 4, 2, 2, parts // 2, 2),
        ("z", "y_hi", "core", "x", "y_lo"),
    )
    return jax.shard_map(
        on_device,
        mesh=fine,
        in_specs=(
            P(DP, TENSOR, None),
            P(DP, TENSOR, None),
            P(),
            P(DP, None, TENSOR),
            P(DP, TENSOR, None),
        ),
        out_specs=(P(DP, TENSOR, None), P(), P(DP, None, TENSOR), P(DP, TENSOR, None)),
        check_vma=False,
    )
```

```python
import functools

import jax
import jax.numpy as jnp
from jax import lax
from jax.experimental import pallas as pl
from jax.experimental.pallas import tpu as pltpu
from jax.sharding import Mesh
from jax.sharding import PartitionSpec as P

NARROW = jnp.bfloat16
WIDE = jnp.float32
LANES = 128
EXTRA = 8
DP = ("z", "y_hi", "core")
TENSOR = ("x", "y_lo")
PLANE = ("y_hi", "x", "y_lo")
COLUMN = ("z", "core")


def dot(a, b, over_a=1, over_b=0):
    return lax.dot_general(a, b, (((over_a,), (over_b,)), ((), ())), preferred_element_type=WIDE)


def iota(shape, dim):
    return lax.broadcasted_iota(jnp.int32, shape, dim)


def pieces(x, count):
    found = []
    for _ in range(count):
        piece = x.astype(NARROW).astype(WIDE)
        found.append(piece)
        x = x - piece
    return found


def as_lanes(columns):
    rows = columns[0].shape[0]
    lane = iota((rows, LANES), 1)
    found = jnp.zeros((rows, LANES), WIDE)
    for k, column in enumerate(columns):
        found = jnp.where(lane == k, column, found)
    return found


def as_lines(columns, width):
    square = as_lanes(columns)
    square = jnp.concatenate([square, jnp.zeros((LANES - square.shape[0], LANES), WIDE)])
    lines = square.T[:EXTRA]
    return jnp.concatenate([lines, jnp.zeros((EXTRA, width - LANES), WIDE)], axis=1)


def as_columns(lines, rows):
    lines = lines[:, :LANES]
    return jnp.concatenate([lines, jnp.zeros((LANES - EXTRA, LANES), WIDE)]).T[:rows]


def selection(size, source):
    return (iota((size, size), 1) == source(iota((size, size), 0))).astype(NARROW)


def turned(size, outer, inner, unit):
    def source(row):
        a = row // unit % outer
        b = row // (unit * outer) % inner
        rest = row // (unit * outer * inner)
        return ((rest * outer + a) * inner + b) * unit + row % unit

    return selection(size, source)


def combine_of(scores):
    weight = jnp.exp(scores - jnp.max(scores, axis=0, keepdims=True))
    return weight / jnp.sum(weight, axis=0, keepdims=True)


def sorted_blocks(both, *sent):
    here = lax.axis_index("x")
    for k, block in enumerate(sent):
        block[...] = both[jnp.bitwise_xor(here, k)]


def image_tokens(blocks):
    seq = blocks[0].shape[0] // 2
    return tuple(
        jnp.concatenate([block[f * seq : (f + 1) * seq, :] for block in blocks]) for f in range(2)
    )


def own_first(mine, other):
    lower = lax.axis_index("core") == 0
    return jnp.concatenate([jnp.where(lower, mine, other), jnp.where(lower, other, mine)])


def cores_rows(rows):
    lower = lax.axis_index("core") == 0
    first, second = rows[: rows.shape[0] // 2], rows[rows.shape[0] // 2 :]
    return jnp.where(lower, first, second), jnp.where(lower, second, first)


def slot_rows(cores, own, *refs):
    router, sent, kept, scores, stats, ordered = refs[-6:]
    gathered = refs[:-6]
    slots, width = router.shape
    half = slots // 2
    tokens, cotangent = image_tokens(gathered)
    order = turned(slots, slots // (cores * own), cores, own)
    ordered[...] = dot(order, router[...]).astype(NARROW)
    logits = dot(ordered[...], tokens, 1, 1)
    scores[...] = logits
    high, low = pieces(jnp.max(logits, axis=1, keepdims=True), 2)
    weight = jnp.exp(logits - (high + low))
    total = jnp.sum(weight, axis=1, keepdims=True)
    stats[...] = as_lanes([high + low, total])
    first, second = (piece.astype(NARROW) for piece in pieces(weight, 2))
    part_in = dot(first, tokens) + dot(second, tokens)
    part_back = dot(combine_of(logits).astype(NARROW), cotangent)
    for k, part in enumerate((part_in, part_back)):
        place = slice(k * half, (k + 1) * half)
        mine, other = cores_rows(part)
        kept[place, :] = mine
        sent[place, :] = other.astype(NARROW)
    sent[slots:, :] = as_lines([high, low, *pieces(total, 2)], width).astype(NARROW)


def joined_rows(unit, arrived, kept, local_stats, both, exact, stats):
    half = exact.shape[0]
    slots = 2 * half
    there = as_columns(arrived[slots:, :].astype(WIDE), slots)
    top_here, total_here = local_stats[:, 0:1], local_stats[:, 1:2]
    top_there, total_there = there[:, 0:1] + there[:, 1:2], there[:, 2:3] + there[:, 3:4]
    top = jnp.maximum(top_here, top_there)
    here, there = jnp.exp(top_here - top), jnp.exp(top_there - top)
    total = here * total_here + there * total_there
    stats[...] = as_lanes([top, total])
    scale_here, _ = cores_rows(here / total)
    scale_there, _ = cores_rows(there / total)
    slot_part = kept[:half, :] * scale_here + arrived[:half, :].astype(WIDE) * scale_there
    back_part = kept[half:, :] + arrived[half:slots, :].astype(WIDE)
    exact[...] = slot_part
    narrow = jnp.concatenate([slot_part, back_part]).astype(NARROW)
    both[...] = dot(turned(slots, 2, half // unit, unit), narrow).astype(NARROW)


def sorted_copies(planes, unit, arrived, sent):
    rows, high = arrived.shape[0], sent.shape[1]
    ordered = dot(turned(rows, rows // (2 * unit), 2 * unit, 1), arrived[...]).astype(NARROW)
    ordered = jnp.concatenate([ordered[: rows // 2], ordered[rows // 2 :]], axis=1)
    for k in range(sent.shape[0]):
        first = k // (sent.shape[0] // planes) * high
        sent[k] = ordered[first : first + high]


def expert_rows(arrived, own, e):
    each = arrived.shape[1] // own
    width = arrived.shape[2] // 2
    return tuple(
        jnp.concatenate(
            [
                arrived[j, e * each : (e + 1) * each, k * width : (k + 1) * width]
                for j in range(arrived.shape[0])
            ]
        )
        for k in range(2)
    )


def experts(arrived, w_in, w_out, sent, acts):
    own, hidden_width = w_in.shape[0], w_in.shape[2]
    each, high, width = acts.shape[0] // own, arrived.shape[1] // own, arrived.shape[2] // 2
    root = (2.0 / jnp.pi) ** 0.5
    for e in range(own):
        mine = slice(e * each, (e + 1) * each)
        there = slice(e * high, (e + 1) * high)
        slot_in, back = expert_rows(arrived, own, e)
        v = dot(slot_in, w_in[e])
        grad_hidden = dot(back, w_out[e], 1, 1)
        t = jnp.tanh(root * (v + 0.044715 * (v * v * v)))
        upper = 0.5 * (1.0 + t)
        low = (v * upper).astype(NARROW)
        slope = upper + 0.5 * v * (1.0 - t * t) * (root * (1.0 + 3 * 0.044715 * (v * v)))
        grad_low = (slope * grad_hidden).astype(NARROW)
        acts[mine, :hidden_width] = low
        acts[mine, hidden_width:] = grad_low
        slot_out = dot(low, w_out[e]).astype(NARROW)
        grad_in = dot(grad_low, w_in[e], 1, 1).astype(NARROW)
        for k in range(sent.shape[0]):
            sent[k, there, :width] = slot_out[k * high : (k + 1) * high]
            sent[k, there, width:] = grad_in[k * high : (k + 1) * high]


def weight_grads(arrived, acts, grad_in, grad_out):
    own, hidden_width = grad_in.shape[0], grad_in.shape[2]
    each = acts.shape[0] // own
    for e in range(own):
        mine = slice(e * each, (e + 1) * each)
        slot_in, back = expert_rows(arrived, own, e)
        grad_in[e] = dot(slot_in, acts[mine, hidden_width:], 0, 0).astype(NARROW)
        grad_out[e] = dot(acts[mine, :hidden_width], back, 0, 0).astype(NARROW)


def joined_results(planes, unit, arrived, both):
    parts, width = arrived.shape[0] // planes, both.shape[1]
    found = []
    for y in range(planes):
        total = arrived[y * parts].astype(WIDE)
        for t in range(1, parts):
            total += arrived[y * parts + t].astype(WIDE)
        found.append(total.astype(NARROW))
    found = jnp.concatenate(found)
    found = jnp.concatenate([found[:, :width], found[:, width:]])
    rows = found.shape[0]
    both[...] = dot(turned(rows, 2 * unit, rows // (2 * unit), 1), found).astype(NARROW)


def dotted_rows(unit, arrived, exact, sent, column):
    half, width = exact.shape
    home = dot(turned(2 * half, half // unit, 2, unit), arrived[...])
    part = jnp.sum(exact[...] * home[half:], axis=1, keepdims=True)
    column[...] = as_lanes([part])
    sent[: 2 * half, :] = home.astype(NARROW)
    sent[2 * half :, :] = as_lines(pieces(part, 3), width).astype(NARROW)


def softmax_grads(cores, own, *refs):
    here, column, there, scores, stats, ordered, left, right, router = refs[-9:]
    gathered = refs[:-9]
    slots = scores.shape[0]
    half = slots // 2
    tokens, cotangent = image_tokens(gathered)
    slot_out = own_first(here[:half, :], there[:half, :])
    grad_in = own_first(here[half:slots, :], there[half:slots, :])
    rest = as_columns(there[slots:, :].astype(WIDE), half)
    column_dot = own_first(column[:, 0:1], rest[:, 0:1] + rest[:, 1:2] + rest[:, 2:3])
    logits = scores[...]
    dispatch = jnp.exp(logits - stats[:, 0:1]) / stats[:, 1:2]
    combine = combine_of(logits)
    grad_combine = dot(slot_out, cotangent, 1, 1)
    grad_dispatch = dot(grad_in, tokens, 1, 1)
    row_dot = jnp.sum(grad_combine * combine, axis=0, keepdims=True)
    grad_logits = (
        combine * (grad_combine - row_dot) + dispatch * (grad_dispatch - column_dot)
    ).astype(NARROW)
    order = turned(slots, cores, slots // (cores * own), own)
    by_slot = dot(dot(order, grad_logits).astype(NARROW), tokens)
    count, high, wide = router.shape
    across = by_slot.shape[1] // wide
    for k in range(count):
        down, over = k // across * high, k % across * wide
        router[k] = by_slot[down : down + high, over : over + wide].astype(NARROW)
    left[:slots, :] = dispatch.astype(NARROW)
    left[slots:, :] = grad_logits
    right[:slots, :] = grad_in
    right[slots:, :] = ordered[...]


def token_grads(left, right, *sent):
    seq = sent[0].shape[0]
    grads = dot(left[...], right[...], 0, 0)
    for k, block in enumerate(sent):
        block[...] = grads[k * seq : (k + 1) * seq].astype(NARROW)


def placed_tokens(*refs):
    arrived, grad_tokens = refs[:-1], refs[-1]
    here = lax.axis_index("x")
    for k, block in enumerate(arrived):
        grad_tokens[jnp.bitwise_xor(here, k)] = block[...]


def summed_copies(arrived, sent):
    total = arrived[0].astype(WIDE)
    for t in range(1, arrived.shape[0]):
        total += arrived[t].astype(WIDE)
    for t in range(sent.shape[0]):
        sent[t] = total.astype(sent.dtype)


def placed(arrived, router):
    count, high, wide = arrived.shape
    across = router.shape[1] // wide
    for k in range(count):
        down, right = k // across * high, k % across * wide
        router[down : down + high, right : right + wide] = arrived[k].astype(router.dtype)


def local(body, outs, flops, *args, limit=12):
    moved = sum(a.size * a.dtype.itemsize for a in (*args, *outs))
    return pl.pallas_call(
        body,
        out_shape=outs,
        in_specs=[pl.BlockSpec(memory_space=pltpu.VMEM)] * len(args),
        out_specs=tuple([pl.BlockSpec(memory_space=pltpu.VMEM)] * len(outs)),
        cost_estimate=pl.CostEstimate(flops=flops, bytes_accessed=moved, transcendentals=0),
        compiler_params=pltpu.CompilerParams(vmem_limit_bytes=limit << 20),
    )(*args)


def shaped(shape, dtype=NARROW):
    return jax.ShapeDtypeStruct(shape, dtype)


def exchanged(blocks, axis):
    return lax.all_to_all(blocks, axis, split_axis=0, concat_axis=0, tiled=True)


def from_partner(block):
    return lax.ppermute(block, "core", [(0, 1), (1, 0)])


def moved(block, k):
    axes = ("core", "x", "y_lo")
    across = lax.axis_size("x")
    pairs = []
    for core in range(2):
        for x in range(across):
            for low in range(2):
                source = (core * across + x) * 2 + low
                pairs.append((source, (low * across + (x ^ k)) * 2 + core))
    return lax.ppermute(block, axes, pairs)


def on_device(tokens, cotangent, dispatch_weight, w_in, w_out):
    images, seq, width = tokens.shape
    slots = dispatch_weight.shape[1]
    own, hidden_width = w_in.shape[0], w_in.shape[2]
    planes, cores = lax.axis_size("y_hi"), lax.axis_size("core")
    plane, column = lax.axis_size(PLANE), lax.axis_size(COLUMN)
    half, count, depth = slots // 2, images * seq, lax.axis_size("z")
    unit = planes * own
    rows = own * images * lax.axis_size(DP)

    both = jnp.concatenate([tokens, cotangent], axis=1)
    blocks = local(
        sorted_blocks, tuple([shaped((2 * seq, width))] * images), count * width, both
    )
    gathered = [moved(block, k) for k, block in enumerate(blocks)]
    sent, kept, scores, stats, ordered = local(
        functools.partial(slot_rows, cores, own),
        (
            shaped((slots + EXTRA, width)),
            shaped((slots, width), WIDE),
            shaped((slots, count), WIDE),
            shaped((slots, LANES), WIDE),
            shaped((slots, width)),
        ),
        8 * slots * count * width,
        *gathered,
        dispatch_weight.T,
    )
    both, exact, stats = local(
        functools.partial(joined_rows, unit),
        (shaped((slots, width)), shaped((half, width), WIDE), shaped((slots, LANES), WIDE)),
        4 * slots * slots * width,
        from_partner(sent),
        kept,
        stats,
    )
    arrived = exchanged(both.reshape(depth, 2 * unit, width), "z").reshape(slots, width)
    high = own * depth
    (sent,) = local(
        functools.partial(sorted_copies, planes, unit),
        (shaped((plane, high, 2 * width)),),
        4 * slots * slots * width,
        arrived,
    )
    arrived = exchanged(sent, PLANE)
    sent, acts = local(
        experts,
        (shaped((plane, high, 2 * width)), shaped((rows, 2 * hidden_width))),
        8 * rows * width * hidden_width,
        arrived,
        w_in,
        w_out,
    )
    back = exchanged(sent, PLANE)
    grad_w_in, grad_w_out = local(
        weight_grads,
        (shaped(w_in.shape), shaped(w_out.shape)),
        4 * rows * width * hidden_width,
        arrived,
        acts,
    )
    (both,) = local(
        functools.partial(joined_results, planes, unit),
        (shaped((slots, width)),),
        4 * slots * slots * width,
        back,
    )
    arrived = exchanged(both.reshape(depth, 2 * unit, width), "z").reshape(slots, width)
    arrived, grad_w_in, grad_w_out = lax.optimization_barrier((arrived, grad_w_in, grad_w_out))
    sent, part = local(
        functools.partial(dotted_rows, unit),
        (shaped((slots + EXTRA, width)), shaped((half, LANES), WIDE)),
        4 * slots * slots * width,
        arrived,
        exact,
    )
    across = width // LANES
    tall = slots * across // plane
    left, right, router = local(
        functools.partial(softmax_grads, cores, own),
        (
            shaped((2 * slots, count)),
            shaped((2 * slots, width)),
            shaped((plane, tall, LANES)),
        ),
        6 * slots * count * width,
        *gathered,
        sent,
        part,
        from_partner(sent),
        scores,
        stats,
        ordered,
    )
    blocks = local(
        token_grads,
        tuple([shaped((seq, width))] * images),
        4 * slots * count * width,
        left,
        right,
    )
    blocks = [moved(block, k) for k, block in enumerate(blocks)]
    (grad_tokens,) = local(
        placed_tokens, (shaped((images, seq, width)),), count * width, *blocks
    )
    (router,) = local(
        summed_copies,
        (shaped((column, tall, LANES)),),
        slots * width,
        exchanged(router, PLANE),
    )
    (router,) = local(
        summed_copies,
        (shaped((plane, tall, LANES)),),
        slots * width,
        exchanged(router, COLUMN),
    )
    (router,) = local(
        placed, (shaped((slots, width), WIDE),), slots * width, exchanged(router, PLANE)
    )
    return (grad_tokens, router.T, grad_w_in, grad_w_out)


def solution(mesh):
    groups, parts = mesh.devices.shape
    fine = Mesh(
        mesh.devices.reshape(groups // 4, 2, 2, parts // 2, 2),
        ("z", "y_hi", "core", "x", "y_lo"),
    )
    return jax.shard_map(
        on_device,
        mesh=fine,
        in_specs=(
            P(DP, TENSOR, None),
            P(DP, TENSOR, None),
            P(),
            P(DP, None, TENSOR),
            P(DP, TENSOR, None),
        ),
        out_specs=(P(DP, TENSOR, None), P(), P(DP, None, TENSOR), P(DP, TENSOR, None)),
        check_vma=False,
    )
```
